32 devices in a mesh: dp: 4 (over z), tensor: 8 (over y, x, core).
Axes of the slice: x: 2, y: 2, z: 4, core: 2. Of those that a mesh axis runs over, the one named last changes fastest.
Arguments:
- gradient: bfloat16 [4, 2560, 8192], P('dp', None, 'tensor'), may hold values from -6 to 6
- feedback: float32 [4, 2560, 8192], P('dp', None, 'tensor'), may hold values from -4 to 4
- q_start: float32 [8192, 32], P('tensor'), may hold values from -6 to 6
Outputs:
- p_factor: float32 [2560, 32], P('tensor')
- q_factor: float32 [8192, 32], P('tensor')
- decoded: float32 [2560, 8192], P(None, 'tensor')
- residual: float32 [4, 2560, 8192], P('dp', None, 'tensor')
The draws below stay inside these ranges and needn't reach their ends.
All inputs are finite; a program needn't handle non-finite values.
Results may differ from the reference program's by a relative error of at most 0.0003.
Values sent between devices are 32-bit elements; how exact they have to be, the bound alone decides.
A program may use at most 64 MiB of HBM per device.

```python
import jax
import jax.numpy as jnp
from jax import lax

DOUT = 2560
DIN = 8192
RANK = 32
REPLICAS = 4
N_DP = 4


def spiked(drawn, own_key, source, target, blocks, factor):
    def block_of(dim):
        return (jnp.arange(drawn.shape[dim]) // (drawn.shape[dim] // blocks)).reshape((-1,) + (1,) * (drawn.ndim - 1 - dim))

    one_side = jax.random.permutation(own_key, blocks)[block_of(target)]
    second = (block_of(target) + blocks // 2) % blocks
    return jnp.where((block_of(source) == one_side) | (block_of(source) == second), factor * drawn, drawn)


def level_of(stream_key, shape, pieces, least, top_value):
    gain = 1.0
    for axis_at, parts in pieces:
        draws = jax.random.uniform(jax.random.fold_in(jax.random.fold_in(stream_key, 6), axis_at), (parts,), jnp.float32, least / len(pieces), top_value / len(pieces))
        gain = gain * jnp.repeat(jnp.exp(draws), shape[axis_at] // parts).reshape((-1,) + (1,) * (len(shape) - 1 - axis_at))
    return gain


def scatter_about(rng, extent, deviation, bound, pieces=(), kind=jnp.bfloat16):
    factor_of = level_of(rng, extent, pieces, -0.22, 0.18) if pieces else 1.0
    drawn = jax.random.normal(rng, extent, jnp.float32) * deviation * factor_of
    return jnp.minimum(jnp.maximum(drawn, -bound), bound).astype(kind)


def heavy_noise(own_key, shape, scale, bound, shards, heavy, held_as=jnp.bfloat16):
    array = scale * jax.random.normal(own_key, shape, jnp.float32)
    if shards:
        array = array * level_of(own_key, shape, shards, -0.22, 0.18)
    return jnp.clip(spiked(array, jax.random.fold_in(own_key, 3), *heavy), -bound, bound).astype(held_as)


def setup_inputs(seed: int = 0) -> dict:
    keys = jax.random.split(jax.random.key(seed), 4)
    return {
        "gradient": heavy_noise(keys[0], (REPLICAS, DOUT, DIN), 1.0, 6.0, ((0, 4), (2, 8)), (2, 1, 8, 2.0)),
        "feedback": scatter_about(keys[1], (REPLICAS, DOUT, DIN), 0.5, 4.0, ((0, 4), (2, 8)), jnp.float32),
        "q_start": scatter_about(keys[2], (DIN, RANK), 1.0, 6.0, ((0, 8),), jnp.float32),
    }


def reference(gradient, feedback, q_start):
    high = lax.Precision.HIGHEST
    merged = gradient.astype(jnp.float32) + feedback
    p_sum = jnp.einsum('rij,jk->ik', merged, q_start, precision=high)
    gram_matrix = jnp.dot(p_sum.T, p_sum, precision=high)
    factor_low = jnp.linalg.cholesky(gram_matrix)
    p_factor = jax.scipy.linalg.solve_triangular(factor_low, p_sum.T, lower=True).T
    q_factor = jnp.einsum('rij,ik->jk', merged, p_factor, precision=high) / N_DP
    decoded = jnp.dot(p_factor, q_factor.T, precision=high)
    residual = merged - decoded[None]
    return (p_factor, q_factor, decoded, residual)
```

```python
import functools

import jax
import jax.numpy as jnp
from jax import lax
from jax.experimental import pallas as pl
from jax.experimental.pallas import tpu as pltpu
from jax.sharding import PartitionSpec as P

MESH = pl.DeviceIdType.MESH
HIGH = lax.Precision.HIGHEST
F32 = jnp.float32
BF16 = jnp.bfloat16
NN = (((1,), (0,)), ((), ()))
NT = (((1,), (1,)), ((), ()))


def dot(a, b, dims, precision=None):
    return lax.dot_general(a, b, dims, precision=precision, preferred_element_type=F32)


def halves(x):
    high = x.astype(BF16)
    return high, (x - high.astype(F32)).astype(BF16)


def inverse_factor(gram):
    rank = gram.shape[0]
    row_at = lax.broadcasted_iota(jnp.int32, (rank, rank), 0)
    col_at = lax.broadcasted_iota(jnp.int32, (rank, rank), 1)
    left = gram
    right = jnp.where(row_at == col_at, 1.0, 0.0).astype(F32)
    for j in range(rank):
        pivot = left[j : j + 1, j : j + 1]
        root = lax.rsqrt(pivot)
        root = root * (1.5 - 0.5 * ((pivot * root) * root))
        left_row = left[j : j + 1, :] * root
        right_row = right[j : j + 1, :] * root
        column = left[:, j : j + 1] * root
        left = left - column * left_row
        right = jnp.where(
            row_at == j, right_row, right - jnp.where(row_at > j, column, 0.0) * right_row
        )
    return right


def factors(n_t, n_dp, g_hbm, f_hbm, q_ref, p_out, q_out, g_buf, f_buf, m_high, m_low, part, part_in,
            chunk, chunk_in, p_all, qpart, qpart_in, q_all, load_g, load_f, s1, r1, s2, r2, s3, r3, s4, r4, s5, r5):
    rank, rows = part.shape[1:]
    width = qpart.shape[2]
    t = lax.axis_index("tensor")
    z = lax.axis_index("dp")

    def block(k):
        return pl.ds(pl.multiple_of(lax.rem(t + k, n_t) * rows, rows), rows)

    def loads(k):
        here = block(k)
        return (
            pltpu.make_async_copy(g_hbm.at[here], g_buf.at[here], load_g.at[k]),
            pltpu.make_async_copy(f_hbm.at[here], f_buf.at[here], load_f.at[k]),
        )

    for k in range(1, n_t + 1):
        for copy in loads(k % n_t):
            copy.start()

    barrier = pltpu.get_barrier_semaphore()
    for k in range(1, n_t):
        pl.semaphore_signal(barrier, inc=1, device_id={"tensor": lax.rem(t + k, n_t)}, device_id_type=MESH)
    for k in range(1, n_dp):
        pl.semaphore_signal(barrier, inc=1, device_id={"dp": lax.rem(z + k, n_dp)}, device_id_type=MESH)

    q_high, q_low = halves(q_ref[...].T)
    q_both = jnp.concatenate([q_high, q_low], axis=0)

    pl.semaphore_wait(barrier, n_t - 1 + n_dp - 1)

    def product(k):
        for copy in loads(k):
            copy.wait()
        here = block(k)
        high, low = halves(g_buf[here, :].astype(F32) + f_buf[here, :])
        m_high[here, :] = high
        m_low[here, :] = low
        first = dot(q_both, high, NT)
        return first[:rank] + first[rank:] + dot(q_high, low, NT)

    def send_part(k):
        peer = lax.rem(t + k, n_t)
        return pltpu.make_async_remote_copy(
            part.at[peer], part_in.at[t], s1.at[peer], r1.at[t], device_id={"tensor": peer}, device_id_type=MESH
        )

    for k in range(1, n_t):
        part[lax.rem(t + k, n_t)] = product(k)
        send_part(k).start()
    part_in[t] = product(0)

    def arrived(buf, sem, slot, axis):
        pltpu.make_async_remote_copy(
            buf.at[slot], buf.at[slot], sem.at[slot], sem.at[slot], device_id={axis: slot}, device_id_type=MESH
        ).wait_recv()

    for k in range(1, n_t):
        arrived(part_in, r1, lax.rem(t + k, n_t), "tensor")
    own = part_in[0]
    for k in range(1, n_t):
        own = own + part_in[k]
    chunk[...] = own
    chunk_in[z] = own

    def send_chunk(k):
        peer = lax.rem(z + k, n_dp)
        return pltpu.make_async_remote_copy(
            chunk, chunk_in.at[z], s2.at[peer], r2.at[z], device_id={"dp": peer}, device_id_type=MESH
        )

    for k in range(1, n_dp):
        send_chunk(k).start()
    for k in range(1, n_dp):
        arrived(chunk_in, r2, lax.rem(z + k, n_dp), "dp")
    own = chunk_in[0]
    for k in range(1, n_dp):
        own = own + chunk_in[k]
    p_all[t] = own

    def send_rows(k):
        peer = lax.rem(t + k, n_t)
        return pltpu.make_async_remote_copy(
            p_all.at[t], p_all.at[t], s3.at[peer], r3.at[t], device_id={"tensor": peer}, device_id_type=MESH
        )

    for k in range(1, n_t):
        send_rows(k).start()
    for k in range(1, n_t):
        arrived(p_all, r3, lax.rem(t + k, n_t), "tensor")
    gram = dot(p_all[0], p_all[0], NT, HIGH)
    for k in range(1, n_t):
        gram = gram + dot(p_all[k], p_all[k], NT, HIGH)
    inverse = inverse_factor(gram)
    for k in range(n_t):
        p_out[k] = dot(inverse, p_all[k], NN, HIGH)

    def q_block(c):
        at = pl.ds(pl.multiple_of(c * width, width), width)
        total = jnp.zeros((rank, width), F32)
        for k in range(n_t):
            high, low = halves(p_out[k])
            both = jnp.concatenate([high, low], axis=0)
            first = dot(both, m_high[k * rows : (k + 1) * rows, at], NN)
            total = total + (first[:rank] + first[rank:] + dot(high, m_low[k * rows : (k + 1) * rows, at], NN))
        return total

    def send_qpart(k):
        peer = lax.rem(z + k, n_dp)
        return pltpu.make_async_remote_copy(
            qpart.at[peer], qpart_in.at[z], s4.at[peer], r4.at[z], device_id={"dp": peer}, device_id_type=MESH
        )

    for k in range(1, n_dp):
        peer = lax.rem(z + k, n_dp)
        qpart[peer] = q_block(peer)
        send_qpart(k).start()
    qpart_in[z] = q_block(z)
    for k in range(1, n_dp):
        arrived(qpart_in, r4, lax.rem(z + k, n_dp), "dp")
    total = qpart_in[0]
    for k in range(1, n_dp):
        total = total + qpart_in[k]
    q_all[z] = total * (1.0 / n_dp)

    def send_q(k):
        peer = lax.rem(z + k, n_dp)
        return pltpu.make_async_remote_copy(
            q_all.at[z], q_all.at[z], s5.at[peer], r5.at[z], device_id={"dp": peer}, device_id_type=MESH
        )

    for k in range(1, n_dp):
        send_q(k).start()
    for k in range(1, n_dp):
        arrived(q_all, r5, lax.rem(z + k, n_dp), "dp")
    for c in range(n_dp):
        q_out[c] = q_all[c]

    for k in range(1, n_t):
        send_part(k).wait_send()
        send_rows(k).wait_send()
    for k in range(1, n_dp):
        send_chunk(k).wait_send()
        send_qpart(k).wait_send()
        send_q(k).wait_send()


def decode(n_dp, g_ref, f_ref, p_ref, q_ref, p_out, q_out, d_out, r_out, q_stack):
    step = pl.program_id(0)
    width = q_ref.shape[2]

    @pl.when(step == 0)
    def _():
        for c in range(n_dp):
            at = slice(c * width, (c + 1) * width)
            high, low = halves(q_ref[c])
            q_stack[:, at] = jnp.concatenate([high, high, low], axis=0)
            q_out[at, :] = q_ref[c].T

    @pl.when(step == lax.axis_index("tensor"))
    def _():
        p_out[...] = p_ref[0].T

    high, low = halves(p_ref[0])
    high, low = high.astype(F32), low.astype(F32)
    p_stack = jnp.concatenate([high, low, high], axis=0).T.astype(BF16)
    decoded = dot(p_stack, q_stack[...], NN)
    d_out[...] = decoded
    r_out[...] = (g_ref[...].astype(F32) + f_ref[...]) - decoded


def kernels(n_t, n_dp, gradient, feedback, q_start):
    gradient, feedback = gradient[0], feedback[0]
    total_rows, cols = gradient.shape
    rank = q_start.shape[1]
    rows, width = total_rows // n_t, cols // n_dp
    vmem = pl.BlockSpec(memory_space=pltpu.VMEM)
    hbm = pl.BlockSpec(memory_space=pl.ANY)
    dma = pltpu.SemaphoreType.DMA
    p3, q4 = pl.pallas_call(
        functools.partial(factors, n_t, n_dp),
        out_shape=(
            jax.ShapeDtypeStruct((n_t, rank, rows), F32),
            jax.ShapeDtypeStruct((n_dp, rank, width), F32),
        ),
        in_specs=[hbm, hbm, vmem],
        out_specs=(vmem, vmem),
        scratch_shapes=[
            pltpu.VMEM((total_rows, cols), BF16),
            pltpu.VMEM((total_rows, cols), F32),
            pltpu.VMEM((total_rows, cols), BF16),
            pltpu.VMEM((total_rows, cols), BF16),
            pltpu.VMEM((n_t, rank, rows), F32),
            pltpu.VMEM((n_t, rank, rows), F32),
            pltpu.VMEM((rank, rows), F32),
            pltpu.VMEM((n_dp, rank, rows), F32),
            pltpu.VMEM((n_t, rank, rows), F32),
            pltpu.VMEM((n_dp, rank, width), F32),
            pltpu.VMEM((n_dp, rank, width), F32),
            pltpu.VMEM((n_dp, rank, width), F32),
            dma((n_t,)), dma((n_t,)),
            dma((n_t,)), dma((n_t,)),
            dma((n_dp,)), dma((n_dp,)),
            dma((n_t,)), dma((n_t,)),
            dma((n_dp,)), dma((n_dp,)),
            dma((n_dp,)), dma((n_dp,)),
        ],
        compiler_params=pltpu.CompilerParams(collective_id=0, has_side_effects=True, vmem_limit_bytes=48 << 20),
    )(gradient, feedback, q_start)
    tile = pl.BlockSpec((rows, cols), lambda i: (i, 0))
    p_factor, q_factor, decoded, residual = pl.pallas_call(
        functools.partial(decode, n_dp),
        grid=(n_t,),
        out_shape=(
            jax.ShapeDtypeStruct((rows, rank), F32),
            jax.ShapeDtypeStruct((cols, rank), F32),
            jax.ShapeDtypeStruct((total_rows, cols), F32),
            jax.ShapeDtypeStruct((total_rows, cols), F32),
        ),
        in_specs=[
            tile,
            tile,
            pl.BlockSpec((1, rank, rows), lambda i: (i, 0, 0)),
            pl.BlockSpec((n_dp, rank, width), lambda i: (0, 0, 0)),
        ],
        out_specs=(
            pl.BlockSpec((rows, rank), lambda i: (0, 0)),
            pl.BlockSpec((cols, rank), lambda i: (0, 0)),
            tile,
            tile,
        ),
        scratch_shapes=[pltpu.VMEM((3 * rank, cols), BF16)],
    )(gradient, feedback, p3, q4)
    return p_factor, q_factor, decoded, residual[None]


def plain(n_t, n_dp, gradient, feedback, q_start):
    merged = gradient[0].astype(F32) + feedback[0]
    row_block = lax.psum_scatter(
        jnp.dot(merged, q_start, precision=HIGH), "tensor", scatter_dimension=0, tiled=True
    )
    row_block = lax.psum(row_block, "dp")
    gram = lax.psum(jnp.dot(row_block.T, row_block, precision=HIGH), "tensor")
    factor_low = jnp.linalg.cholesky(gram)
    p_factor = jax.scipy.linalg.solve_triangular(factor_low, row_block.T, lower=True).T
    basis_all = lax.all_gather(p_factor, "tensor", axis=0, tiled=True)
    q_local = lax.dot_general(merged, basis_all, (((0,), (0,)), ((), ())), precision=HIGH)
    q_factor = lax.psum(q_local, "dp") / n_dp
    decoded = jnp.dot(basis_all, q_factor.T, precision=HIGH)
    return p_factor, q_factor, decoded, (merged - decoded)[None]


def local(n_t, n_dp, gradient, feedback, q_start):
    total_rows, cols = gradient.shape[1:]
    fits = total_rows % (16 * n_t) == 0 and cols % (128 * n_dp) == 0 and q_start.shape[1] % 16 == 0
    small = total_rows * cols * 10 <= 36 << 20
    return (kernels if fits and small else plain)(n_t, n_dp, gradient, feedback, q_start)


def solution(mesh):
    n_t, n_dp = mesh.shape["tensor"], mesh.shape["dp"]
    in_specs = (P("dp", None, "tensor"), P("dp", None, "tensor"), P("tensor", None))
    out_specs = (P("tensor", None), P("tensor", None), P(None, "tensor"), P("dp", None, "tensor"))
    step = functools.partial(local, n_t, n_dp)
    return jax.shard_map(step, mesh=mesh, in_specs=in_specs, out_specs=out_specs, check_vma=False)
```

```python
import functools

import jax
import jax.numpy as jnp
from jax import lax
from jax.experimental import pallas as pl
from jax.experimental.pallas import tpu as pltpu
from jax.sharding import PartitionSpec as P

MESH = pl.DeviceIdType.MESH
HIGH = lax.Precision.HIGHEST
F32 = jnp.float32
BF16 = jnp.bfloat16
NN = (((1,), (0,)), ((), ()))
NT = (((1,), (1,)), ((), ()))


def dot(a, b, dims, precision=None):
    return lax.dot_general(a, b, dims, precision=precision, preferred_element_type=F32)


def halves(x):
    high = x.astype(BF16)
    return high, (x - high.astype(F32)).astype(BF16)


def inverse_factor(gram):
    rank = gram.shape[0]
    row_at = lax.broadcasted_iota(jnp.int32, (rank, rank), 0)
    col_at = lax.broadcasted_iota(jnp.int32, (rank, rank), 1)
    left = gram
    right = jnp.where(row_at == col_at, 1.0, 0.0).astype(F32)
    for j in range(rank):
        pivot = left[j : j + 1, j : j + 1]
        root = lax.rsqrt(pivot)
        root = root * (1.5 - 0.5 * ((pivot * root) * root))
        left_row = left[j : j + 1, :] * root
        right_row = right[j : j + 1, :] * root
        column = left[:, j : j + 1] * root
        left = left - column * left_row
        right = jnp.where(
            row_at == j, right_row, right - jnp.where(row_at > j, column, 0.0) * right_row
        )
    return right


def factors(n_t, n_dp, g_ref, f_hbm, q_ref, p_own, p_out, q_out, m_out, m_high, m_low, part, part_in,
            chunk, chunk_in, p_all, p_sum, qpart, qpart_in, q_all, load_f, s1, r1, s2, r2, s3, r3, s4, r4, s5, r5):
    rank, rows = part.shape[1:]
    width = qpart.shape[2]
    t = lax.axis_index("tensor")
    z = lax.axis_index("dp")

    def block(k):
        return pl.ds(pl.multiple_of(lax.rem(t + k, n_t) * rows, rows), rows)

    def load(k):
        here = block(k)
        return pltpu.make_async_copy(f_hbm.at[here], m_out.at[here], load_f.at[k])

    for k in range(1, n_t + 1):
        load(k % n_t).start()

    barrier = pltpu.get_barrier_semaphore()
    for k in range(1, n_t):
        pl.semaphore_signal(barrier, inc=1, device_id={"tensor": lax.rem(t + k, n_t)}, device_id_type=MESH)
    for k in range(1, n_dp):
        pl.semaphore_signal(barrier, inc=1, device_id={"dp": lax.rem(z + k, n_dp)}, device_id_type=MESH)

    q_high, q_low = halves(q_ref[...])
    q_both = jnp.concatenate([q_high, q_low], axis=0)

    pl.semaphore_wait(barrier, n_t - 1 + n_dp - 1)

    def product(k):
        load(k).wait()
        here = block(k)
        merged = g_ref[here, :].astype(F32) + m_out[here, :]
        m_out[here, :] = merged
        high, low = halves(merged)
        m_high[here, :] = high
        m_low[here, :] = low
        first = dot(q_both, high, NT)
        return first[:rank] + first[rank:] + dot(q_high, low, NT)

    def send_part(k):
        peer = lax.rem(t + k, n_t)
        return pltpu.make_async_remote_copy(
            part.at[peer], part_in.at[t], s1.at[peer], r1.at[t], device_id={"tensor": peer}, device_id_type=MESH
        )

    for k in range(1, n_t):
        part[lax.rem(t + k, n_t)] = product(k)
        send_part(k).start()
    part_in[t] = product(0)

    def arrived(buf, sem, slot, axis):
        pltpu.make_async_remote_copy(
            buf.at[slot], buf.at[slot], sem.at[slot], sem.at[slot], device_id={axis: slot}, device_id_type=MESH
        ).wait_recv()

    for k in range(1, n_t):
        arrived(part_in, r1, lax.rem(t + k, n_t), "tensor")
    own = part_in[0]
    for k in range(1, n_t):
        own = own + part_in[k]
    chunk[...] = own
    chunk_in[z] = own

    def send_chunk(k):
        peer = lax.rem(z + k, n_dp)
        return pltpu.make_async_remote_copy(
            chunk, chunk_in.at[z], s2.at[peer], r2.at[z], device_id={"dp": peer}, device_id_type=MESH
        )

    for k in range(1, n_dp):
        send_chunk(k).start()
    for k in range(1, n_dp):
        arrived(chunk_in, r2, lax.rem(z + k, n_dp), "dp")
    own = chunk_in[0]
    for k in range(1, n_dp):
        own = own + chunk_in[k]
    p_all[t] = own

    def send_rows(k):
        peer = lax.rem(t + k, n_t)
        return pltpu.make_async_remote_copy(
            p_all.at[t], p_all.at[t], s3.at[peer], r3.at[t], device_id={"tensor": peer}, device_id_type=MESH
        )

    for k in range(1, n_t):
        send_rows(k).start()
    for k in range(1, n_t):
        arrived(p_all, r3, lax.rem(t + k, n_t), "tensor")
    for k in range(n_t):
        p_sum[:, k * rows : (k + 1) * rows] = p_all[k]
    inverse = inverse_factor(dot(p_sum[...], p_sum[...], NT, HIGH))
    p_own[...] = dot(inverse, p_all[t], NN, HIGH)
    factor = dot(inverse, p_sum[...], NN, HIGH)
    p_out[...] = factor
    p_high, p_low = halves(factor)
    p_both = jnp.concatenate([p_high, p_low], axis=0)

    def q_block(c):
        at = pl.ds(pl.multiple_of(c * width, width), width)
        first = dot(p_both, m_high[:, at], NN)
        return first[:rank] + first[rank:] + dot(p_high, m_low[:, at], NN)

    def send_qpart(k):
        peer = lax.rem(z + k, n_dp)
        return pltpu.make_async_remote_copy(
            qpart.at[peer], qpart_in.at[z], s4.at[peer], r4.at[z], device_id={"dp": peer}, device_id_type=MESH
        )

    for k in range(1, n_dp):
        peer = lax.rem(z + k, n_dp)
        qpart[peer] = q_block(peer)
        send_qpart(k).start()
    qpart_in[z] = q_block(z)
    for k in range(1, n_dp):
        arrived(qpart_in, r4, lax.rem(z + k, n_dp), "dp")
    total = qpart_in[0]
    for k in range(1, n_dp):
        total = total + qpart_in[k]
    q_all[z] = total * (1.0 / n_dp)

    def send_q(k):
        peer = lax.rem(z + k, n_dp)
        return pltpu.make_async_remote_copy(
            q_all.at[z], q_all.at[z], s5.at[peer], r5.at[z], device_id={"dp": peer}, device_id_type=MESH
        )

    for k in range(1, n_dp):
        send_q(k).start()
    for k in range(1, n_dp):
        arrived(q_all, r5, lax.rem(z + k, n_dp), "dp")
    for c in range(n_dp):
        q_out[:, c * width : (c + 1) * width] = q_all[c]

    for k in range(1, n_t):
        send_part(k).wait_send()
        send_rows(k).wait_send()
    for k in range(1, n_dp):
        send_chunk(k).wait_send()
        send_qpart(k).wait_send()
        send_q(k).wait_send()


def decode(m_ref, own_ref, p_ref, q_ref, p_out, q_out, d_out, r_out, q_stack):
    step = pl.program_id(0)
    rows = d_out.shape[0]
    here = pl.ds(pl.multiple_of(step * rows, rows), rows)

    @pl.when(step == 0)
    def _():
        high, low = halves(q_ref[...])
        q_stack[...] = jnp.concatenate([high, high, low], axis=0)
        q_out[...] = q_ref[...]
        p_out[...] = own_ref[...]

    high, low = halves(p_ref[:, here])
    high, low = high.astype(F32), low.astype(F32)
    p_stack = jnp.concatenate([high, low, high], axis=0).T.astype(BF16)
    decoded = dot(p_stack, q_stack[...], NN)
    d_out[...] = decoded
    r_out[...] = m_ref[here, :] - decoded


def kernels(n_t, n_dp, gradient, feedback, q_start):
    gradient, feedback = gradient[0], feedback[0]
    total_rows, cols = gradient.shape
    rank = q_start.shape[1]
    rows, width = total_rows // n_t, cols // n_dp
    vmem = pl.BlockSpec(memory_space=pltpu.VMEM)
    hbm = pl.BlockSpec(memory_space=pltpu.HBM)
    dma = pltpu.SemaphoreType.DMA
    own, basis, right, merged = pl.pallas_call(
        functools.partial(factors, n_t, n_dp),
        out_shape=(
            jax.ShapeDtypeStruct((rank, rows), F32),
            jax.ShapeDtypeStruct((rank, total_rows), F32),
            jax.ShapeDtypeStruct((rank, cols), F32),
            jax.ShapeDtypeStruct((total_rows, cols), F32),
        ),
        in_specs=[vmem, hbm, vmem],
        out_specs=(vmem, vmem, vmem, vmem),
        scratch_shapes=[
            pltpu.VMEM((total_rows, cols), BF16),
            pltpu.VMEM((total_rows, cols), BF16),
            pltpu.VMEM((n_t, rank, rows), F32),
            pltpu.VMEM((n_t, rank, rows), F32),
            pltpu.VMEM((rank, rows), F32),
            pltpu.VMEM((n_dp, rank, rows), F32),
            pltpu.VMEM((n_t, rank, rows), F32),
            pltpu.VMEM((rank, total_rows), F32),
            pltpu.VMEM((n_dp, rank, width), F32),
            pltpu.VMEM((n_dp, rank, width), F32),
            pltpu.VMEM((n_dp, rank, width), F32),
            dma((n_t,)),
            dma((n_t,)), dma((n_t,)),
            dma((n_dp,)), dma((n_dp,)),
            dma((n_t,)), dma((n_t,)),
            dma((n_dp,)), dma((n_dp,)),
            dma((n_dp,)), dma((n_dp,)),
        ],
        compiler_params=pltpu.CompilerParams(collective_id=0, has_side_effects=True, vmem_limit_bytes=30 << 20),
    )(gradient, feedback, q_start.T)
    tile = pl.BlockSpec((256, cols), lambda i: (i, 0))
    p_factor, q_factor, decoded, residual = pl.pallas_call(
        decode,
        grid=(total_rows // 256,),
        out_shape=(
            jax.ShapeDtypeStruct((rank, rows), F32),
            jax.ShapeDtypeStruct((rank, cols), F32),
            jax.ShapeDtypeStruct((total_rows, cols), F32),
            jax.ShapeDtypeStruct((total_rows, cols), F32),
        ),
        in_specs=[vmem, vmem, vmem, vmem],
        out_specs=(
            pl.BlockSpec((rank, rows), lambda i: (0, 0)),
            pl.BlockSpec((rank, cols), lambda i: (0, 0)),
            tile,
            tile,
        ),
        scratch_shapes=[pltpu.VMEM((3 * rank, cols), BF16)],
        compiler_params=pltpu.CompilerParams(vmem_limit_bytes=24 << 20),
    )(merged, own, basis, right)
    return p_factor.T, q_factor.T, decoded, residual[None]


def plain(n_t, n_dp, gradient, feedback, q_start):
    merged = gradient[0].astype(F32) + feedback[0]
    row_block = lax.psum_scatter(
        jnp.dot(merged, q_start, precision=HIGH), "tensor", scatter_dimension=0, tiled=True
    )
    row_block = lax.psum(row_block, "dp")
    gram = lax.psum(jnp.dot(row_block.T, row_block, precision=HIGH), "tensor")
    factor_low = jnp.linalg.cholesky(gram)
    p_factor = jax.scipy.linalg.solve_triangular(factor_low, row_block.T, lower=True).T
    basis_all = lax.all_gather(p_factor, "tensor", axis=0, tiled=True)
    q_local = lax.dot_general(merged, basis_all, (((0,), (0,)), ((), ())), precision=HIGH)
    q_factor = lax.psum(q_local, "dp") / n_dp
    decoded = jnp.dot(basis_all, q_factor.T, precision=HIGH)
    return p_factor, q_factor, decoded, (merged - decoded)[None]


def local(n_t, n_dp, gradient, feedback, q_start):
    total_rows, cols = gradient.shape[1:]
    fits = total_rows % (16 * n_t) == 0 and total_rows % 256 == 0 and cols % (128 * n_dp) == 0 and q_start.shape[1] % 16 == 0
    small = total_rows * cols * 10 <= 36 << 20
    return (kernels if fits and small else plain)(n_t, n_dp, gradient, feedback, q_start)


def solution(mesh):
    n_t, n_dp = mesh.shape["tensor"], mesh.shape["dp"]
    in_specs = (P("dp", None, "tensor"), P("dp", None, "tensor"), P("tensor", None))
    out_specs = (P("tensor", None), P("tensor", None), P(None, "tensor"), P("dp", None, "tensor"))
    step = functools.partial(local, n_t, n_dp)
    return jax.shard_map(step, mesh=mesh, in_specs=in_specs, out_specs=out_specs, check_vma=False)
```
